256 devices in a mesh: rel: 8 (over x, z_lo), ent: 32 (over z_hi, y, core).
Axes of the slice: x: 4, y: 4, z: 8 (z_hi: 4, z_lo: 2; z = z_hi * 2 + z_lo), core: 2. Of those that a mesh axis runs over, the one named last changes fastest.
Arguments:
- state: bfloat16 [8192, 1024], P('ent', 'rel'), may hold values from -4 to 4
- rel_weight: bfloat16 [24, 1024, 1024], P('rel', 'ent'), may hold values from -0.0390625 to 0.0390625
- gate_weight: bfloat16 [1024, 1024], P(None, 'rel'), may hold values from -0.1875 to 0.1875
- gate_bias: float32 [1024], P('rel'), may hold values from -4 to 4
- update_bias: float32 [1024], P('rel'), may hold values from -3 to 3
- tile_values: bfloat16 [8, 512, 128, 128], P('rel', 'ent'), may hold values from 0 to 0.119628906
- tile_index: int32 [8, 3, 512], P('rel', None, 'ent'), may hold values from 0 to 63, as said below
- tile_count: int32 [8, 32], P('rel', 'ent'), may hold values from 1 to 16, as said below
Outputs:
- new_state: bfloat16 [8192, 1024], P('ent', 'rel')
The draws below stay inside these ranges and needn't reach their ends.
Inputs may be any that keep to these rules, and one draw needn't show every extreme that they name: `tile_index`: row 0 names a source tile of the whole graph, row 1 a destination tile of the partition that owns the slot (below 2), row 2 a relation within the group (below 3). `tile_count`: slots of a partition at or past its count are padding; in every group some partition fills all 16 slots.
All inputs are finite; a program needn't handle non-finite values.
Results may differ from the reference program's by a relative error of at most 0.0065.
Values may be sent and summed in bfloat16 or wider, within the bound.
A program may use at most 128 MiB of HBM per device.

```python
import jax
import jax.numpy as jnp
from jax import lax

H = 1024
RELS = 24
TILE = 128
LAYERS = 1
ENT_DEV = 256
SLOTS = 16
GROUPS = 8
PARTS_SIZE = 32
NODES = 8192
LISTED = 512
N_REL = 8
N_ENT = 32


def draw_tile_index(key, part):
    keys = jax.random.split(jax.random.fold_in(key, 11), 3)
    source = jax.random.randint(keys[0], (GROUPS, LISTED), 0, NODES // TILE, dtype=jnp.int32)
    target = jax.random.randint(keys[1], (GROUPS, LISTED), 0, ENT_DEV // TILE, dtype=jnp.int32)
    relation = jax.random.randint(keys[2], (GROUPS, LISTED), 0, RELS // GROUPS, dtype=jnp.int32)
    return jnp.stack([source, target, relation], axis=1)


def draw_tile_count(key, part):
    keys = jax.random.split(jax.random.fold_in(key, 23), 2)
    counts = jax.random.randint(keys[0], (GROUPS, PARTS_SIZE), 1, SLOTS + 1, dtype=jnp.int32)
    chosen = jax.random.randint(keys[1], (GROUPS, 1), 0, PARTS_SIZE, dtype=jnp.int32)
    spots = jnp.arange(PARTS_SIZE, dtype=jnp.int32)[None, :] == chosen
    return jnp.where(spots, SLOTS, counts).astype(jnp.int32)


def block_levels(rng, dims, cuts, low, high):
    loudness = 1.0
    for dim, parts in cuts:
        heights = jax.random.uniform(jax.random.fold_in(jax.random.fold_in(rng, 6), dim), (parts,), jnp.float32, low / len(cuts), high / len(cuts))
        loudness = loudness * jnp.repeat(jnp.exp(heights), dims[dim] // parts).reshape((-1,) + (1,) * (len(dims) - 1 - dim))
    return loudness


def bell_draw(own_key, dims, scale, bound, shards=(), held_as=jnp.bfloat16):
    drawn = jax.random.normal(own_key, dims, jnp.float32) * scale
    if len(shards) > 0:
        drawn = block_levels(own_key, dims, shards, -0.22, 0.18) * drawn
    return jnp.clip(drawn, min=-bound, max=bound).astype(held_as)


def setup_inputs(seed: int = 0) -> dict:
    key_list = jax.random.split(jax.random.key(seed), 9)
    state = bell_draw(key_list[0], (NODES, H), 1.0, 4.0, ((0, 32), (1, 8)))
    rel_weight = bell_draw(key_list[1], (RELS, H, H), (H * RELS) ** -0.5, 0.0390625, ((0, 8), (1, 32)))
    gate_weight = bell_draw(key_list[2], (H, H), H ** -0.5, 0.1875, ((1, 8),))
    gate_bias = bell_draw(key_list[3], (H,), 1.0, 4.0, ((0, 8),), jnp.float32)
    update_bias = bell_draw(key_list[4], (H,), 0.7, 3.0, ((0, 8),), jnp.float32)
    tile_values = jnp.clip(0.119628906 * jax.random.uniform(key_list[5], (GROUPS, LISTED, TILE, TILE), jnp.float32) ** block_levels(key_list[5], (GROUPS, LISTED, TILE, TILE), ((0, 8), (1, 32)), -0.2, 0.2), 0.0, 0.119628906).astype(jnp.bfloat16)
    tile_index = draw_tile_index(jax.random.fold_in(key_list[8], 71), 0)
    tile_count = draw_tile_count(jax.random.fold_in(key_list[8], 71), 0)
    return {"state": state, "rel_weight": rel_weight, "gate_weight": gate_weight, "gate_bias": gate_bias, "update_bias": update_bias, "tile_values": tile_values, "tile_index": tile_index, "tile_count": tile_count}


def aggregate_tiles(hidden, values, listing, live_total, rel_dev, per_tile):
    features = hidden.shape[1]
    sources = hidden.reshape(-1, TILE, features)[listing[0]]
    product = jnp.einsum("sij,sjh->sih", values.astype(jnp.float32), sources.astype(jnp.float32))
    slot_ids = jnp.arange(listing.shape[1], dtype=jnp.int32)
    live_mask = (slot_ids < live_total).astype(jnp.float32)
    target = listing[1] * rel_dev + listing[2]
    classes = jnp.arange(per_tile * rel_dev, dtype=jnp.int32)
    select = (target[:, None] == classes[None, :]).astype(jnp.float32) * live_mask[:, None]
    summed = jnp.einsum("sk,sih->kih", select, product, precision=lax.Precision.HIGHEST)
    return summed.astype(jnp.bfloat16).reshape(per_tile, rel_dev, TILE, features)


def reference(state, rel_weight, gate_weight, gate_bias, update_bias, tile_values, tile_index, tile_count):
    rel_dev = RELS // N_REL
    per_tile = ENT_DEV // TILE
    hidden = state
    for layer_num in range(LAYERS):
        def partition(part_num):
            summed = jnp.zeros((ENT_DEV, H), jnp.float32)
            for group in range(N_REL):
                first_slot = part_num * SLOTS
                values = lax.dynamic_slice_in_dim(tile_values[group], first_slot, SLOTS, 0)
                listing = lax.dynamic_slice_in_dim(tile_index[group], first_slot, SLOTS, 1)
                live_total = tile_count[group][part_num]
                aggregate = aggregate_tiles(hidden, values, listing, live_total, rel_dev, per_tile)
                weights = rel_weight[group * rel_dev:(group + 1) * rel_dev].astype(jnp.float32)
                term = jnp.einsum("drih,rhk->dik", aggregate.astype(jnp.float32), weights)
                summed = summed + term.reshape(ENT_DEV, H)
            return summed

        message = lax.map(partition, jnp.arange(N_ENT, dtype=jnp.int32)).reshape(NODES, H)
        gate_open = jax.nn.sigmoid(jnp.dot(hidden, gate_weight, preferred_element_type=jnp.float32) + gate_bias)
        update = jnp.tanh(message + update_bias)
        hidden = ((1.0 - gate_open) * hidden.astype(jnp.float32) + gate_open * update).astype(jnp.bfloat16)
    return hidden
```

```python
import jax
import jax.numpy as jnp
from jax import lax
from jax.experimental import pallas as pl
from jax.experimental.pallas import tpu as pltpu

MESH = pl.DeviceIdType.MESH
BF = jnp.bfloat16
F32 = jnp.float32


class Sems:
    def __init__(self):
        self.total = 0

    def take(self, count):
        first = self.total
        self.total += count
        return first


S = Sems()
TVP, TVM, TVR = S.take(2), S.take(2), S.take(2)
MET = S.take(3)
SY, SYR = S.take(2), S.take(2)
SZP, SZM = S.take(4), S.take(4)
SD = S.take(8)
GP, GM, GR = S.take(2), S.take(2), S.take(2)
WZP, WZM, WZR0, WZR1 = S.take(3), S.take(3), S.take(3), S.take(3)
WX = S.take(9)
WYP, WYM, WYR0, WYR1 = S.take(12), S.take(12), S.take(12), S.take(12)
WD = S.take(16)
PT = S.take(8)


def kernel(
    meta_in, state_in, relw_in, tv_in, gw_ref, gb_ref, ub_ref, out_ref,
    tvb, metav, metas, sb, rb, wz, wb, lhs, rhs, ab, pb, qb, ssem, rsem, lsem,
):
    rel = lax.axis_index("rel")
    ent = lax.axis_index("ent")
    x, zl = lax.div(rel, 2), lax.rem(rel, 2)
    zh, y, c = lax.div(ent, 8), lax.rem(lax.div(ent, 2), 4), lax.rem(ent, 2)
    z = zh * 2 + zl

    def turn(v, step, count):
        return lax.rem(v + (step + count) % count, count)

    def at(x_=None, y_=None, z_=None, c_=None):
        xx = x if x_ is None else x_
        yy = y if y_ is None else y_
        zz = z if z_ is None else z_
        cc = c if c_ is None else c_
        return (xx * 2 + lax.rem(zz, 2), lax.div(zz, 2) * 8 + yy * 2 + cc)

    xp, xm, x2 = turn(x, 1, 4), turn(x, -1, 4), turn(x, 2, 4)
    yp, ym, y2 = turn(y, 1, 4), turn(y, -1, 4), turn(y, 2, 4)
    hp, hm, h2 = turn(zh, 1, 4), turn(zh, -1, 4), turn(zh, 2, 4)
    zo = zh * 2 + (1 - zl)
    dxp, dxm, dx2 = at(x_=xp), at(x_=xm), at(x_=x2)
    dyp, dym = at(y_=yp), at(y_=ym)
    dzp, dzm = at(z_=turn(z, 1, 8)), at(z_=turn(z, -1, 8))
    dhp, dhm = at(z_=hp * 2 + zl), at(z_=hm * 2 + zl)
    dco = at(c_=1 - c)
    peers = [dxp, dxm, dx2, dyp, dym, dzp, dzm, dhp, dhm, dco]
    peers += [at(x_=v, z_=zo) for v in (xp, xm, x2)]

    pending = []

    def copy(i, src, dst, dev):
        return pltpu.make_async_remote_copy(
            src_ref=src, dst_ref=dst, send_sem=ssem.at[i], recv_sem=rsem.at[i],
            device_id=dev, device_id_type=MESH,
        )

    def send(i, src, dst, dev):
        d = copy(i, src, dst, dev)
        d.start()
        pending.append(d)

    def got(i, ref):
        copy(i, ref, ref, dco).wait_recv()

    yc = y * 2 + c
    own_t = ((zh * 2 + c) * 4 + y) * 2
    row0 = (zh * 2 + c) * 8

    local = [
        pltpu.make_async_copy(relw_in, wz.at[zh], lsem.at[0]),
        pltpu.make_async_copy(state_in, sb.at[zl, pl.ds(own_t, 2)], lsem.at[1]),
        pltpu.make_async_copy(meta_in, metav.at[x], lsem.at[2]),
        pltpu.make_async_copy(tv_in, tvb.at[x], lsem.at[3]),
    ]
    for d in local:
        d.start()
    barrier = pltpu.get_barrier_semaphore()
    for dev in peers:
        pl.semaphore_signal(barrier, inc=1, device_id=dev, device_id_type=MESH)
    for d in local:
        d.wait()
    pl.semaphore_wait(barrier, len(peers))

    for r in range(3):
        send(WZP + r, wz.at[zh, r], wz.at[zh, r], dhp)
        send(WZM + r, wz.at[zh, r], wz.at[zh, r], dhm)
    mine = sb.at[zl, pl.ds(own_t, 2)]
    send(SY, mine, mine, dyp)
    send(SY + 1, mine, mine, dym)
    for k, dev in enumerate((dxp, dxm, dx2)):
        send(MET + k, metav.at[x], metav.at[x], dev)

    def weight_row(slot, r):
        d = lax.rem(slot - x + 4, 4)

        @pl.when(d != 0)
        def _():
            copy(
                WX + (d - 1) * 3 + r, wz.at[slot, r], wb.at[x, r, yc], at(x_=slot)
            ).start()

    for r in range(3):
        weight_row(zh, r)

    def tv_half(x_, h):
        return tvb.at[x_, pl.ds(h * 8, 8)]

    send(TVP, tv_half(x, 0), tv_half(x, 0), dxp)
    send(TVM + 1, tv_half(x, 1), tv_half(x, 1), dxm)

    def piece(y_, first, count):
        return sb.at[zl, pl.ds(row0 + y_ * 2 + first, count)]

    got(SY, piece(ym, 0, 2))
    send(SYR, piece(ym, 0, 1), piece(ym, 0, 1), dyp)
    got(SY + 1, piece(yp, 0, 2))
    send(SYR + 1, piece(yp, 1, 1), piece(yp, 1, 1), dym)

    for r in range(3):
        got(WZP + r, wz.at[hm, r])
        half = wz.at[hm, r, pl.ds(0, 16)]
        send(WZR0 + r, half, half, dhp)
        got(WZM + r, wz.at[hp, r])
        half = wz.at[hp, r, pl.ds(16, 16)]
        send(WZR1 + r, half, half, dhm)
        weight_row(hm, r)
        weight_row(hp, r)

    got(SYR, piece(y2, 0, 1))
    got(SYR + 1, piece(y2, 1, 1))

    def chunk(step, cc, first=0, count=8):
        zz = turn(z, step, 8)
        return sb.at[lax.rem(zz, 2), pl.ds((lax.div(zz, 2) * 2 + cc) * 8 + first, count)]

    def share(k, step):
        send(SD + k, chunk(step, c), chunk(step, c), dco)

    send(SZP, chunk(0, c), chunk(0, c), dzp)
    send(SZM, chunk(0, c), chunk(0, c), dzm)
    share(0, 0)

    for r in range(3):
        got(WZR0 + r, wz.at[h2, r, pl.ds(0, 16)])
        got(WZR1 + r, wz.at[h2, r, pl.ds(16, 16)])
        weight_row(h2, r)

    def block(d, r, y_, cc=None):
        return wb.at[turn(x, -d, 4), r, y_ * 2 + (c if cc is None else cc)]

    def half_block(d, r, y_, h):
        return wb.at[turn(x, -d, 4), r, y_ * 2 + c, pl.ds(h * 16, 16)]

    def whole_block(d, y_, cc=None):
        return wb.at[turn(x, -d, 4), :, y_ * 2 + (c if cc is None else cc)]

    for r in range(3):
        send(WYP + r, wz.at[x, r], block(0, r, y), dyp)
        send(WYM + r, wz.at[x, r], block(0, r, y), dym)
    send(WD, wz.at[x], whole_block(0, y), dco)
    wb[x, :, yc] = wz[x]

    def weights_out(d):
        for r in range(3):
            got(WX + (d - 1) * 3 + r, block(d, r, y))
            send(WYP + d * 3 + r, block(d, r, y), block(d, r, y), dyp)
            send(WYM + d * 3 + r, block(d, r, y), block(d, r, y), dym)
        send(WD + d, whole_block(d, y), whole_block(d, y), dco)

    def weights_on(d):
        for r in range(3):
            got(WYP + d * 3 + r, block(d, r, ym))
            send(WYR0 + d * 3 + r, half_block(d, r, ym, 0), half_block(d, r, ym, 0), dyp)
            got(WYM + d * 3 + r, block(d, r, yp))
            send(WYR1 + d * 3 + r, half_block(d, r, yp, 1), half_block(d, r, yp, 1), dym)
        send(WD + 4 + d, whole_block(d, ym), whole_block(d, ym), dco)
        send(WD + 8 + d, whole_block(d, yp), whole_block(d, yp), dco)

    def weights_end(d):
        for r in range(3):
            got(WYR0 + d * 3 + r, half_block(d, r, y2, 0))
            got(WYR1 + d * 3 + r, half_block(d, r, y2, 1))
        send(WD + 12 + d, whole_block(d, y2), whole_block(d, y2), dco)

    def state_on(k):
        got(SZP + k - 1, chunk(-k, c))
        got(SZM + k - 1, chunk(k, c))
        if k < 3:
            send(SZP + k, chunk(-k, c), chunk(-k, c), dzp)
            send(SZM + k, chunk(k, c), chunk(k, c), dzm)
        else:
            send(SZP + k, chunk(-k, c, 0, 4), chunk(-k, c, 0, 4), dzp)
            send(SZM + k, chunk(k, c, 4, 4), chunk(k, c, 4, 4), dzm)
        share(2 * k - 1, -k)
        share(2 * k, k)

    weights_out(1)
    weights_out(3)
    state_on(1)
    for q in range(2):
        pair = sb.at[q, pl.ds(own_t, 2)]
        send(GP + q, pair, rb.at[x, q], dxp)
        send(GM + q, pair, rb.at[x, q], dxm)
    weights_out(2)
    send(TVP + 1, tv_half(x, 1), tv_half(x, 1), dxp)
    send(TVM, tv_half(x, 0), tv_half(x, 0), dxm)
    weights_on(0)
    state_on(2)
    got(TVP, tv_half(xm, 0))
    send(TVR, tv_half(xm, 0), tv_half(xm, 0), dxp)
    got(TVM + 1, tv_half(xp, 1))
    send(TVR + 1, tv_half(xp, 1), tv_half(xp, 1), dxm)
    weights_on(1)
    state_on(3)
    weights_on(3)
    weights_end(0)
    for q in range(2):
        got(GP + q, rb.at[xm, q])
        got(GM + q, rb.at[xp, q])
    send(GR, rb.at[xm, 0], rb.at[xm, 0], dxp)
    send(GR + 1, rb.at[xp, 1], rb.at[xp, 1], dxm)
    got(SZP + 3, chunk(4, c, 0, 4))
    got(SZM + 3, chunk(4, c, 4, 4))
    share(7, 4)
    weights_on(2)
    for k, v in enumerate((xm, xp, x2)):
        got(MET + k, metav.at[v])
    listing = pltpu.make_async_copy(metav, metas, lsem.at[4])
    listing.start()
    got(TVP + 1, tv_half(xm, 1))
    got(TVM, tv_half(xp, 0))
    got(TVR, tv_half(x2, 0))
    got(TVR + 1, tv_half(x2, 1))
    for k, step in enumerate((0, -1, 1, -2, 2, -3, 3, 4)):
        got(SD + k, chunk(step, 1 - c))
    listing.wait()

    def products(group, carry):
        for s in range(16):
            src = metas[group, 0, s]
            cls = metas[group, 1, s]
            rhs[s * 128 : (s + 1) * 128, 0:128] = sb[0, src]
            rhs[s * 128 : (s + 1) * 128, 128:256] = sb[1, src]
            values = tvb[group, s].astype(F32)
            for k in range(6):
                on = jnp.where(cls == k, 1.0, 0.0).astype(F32)
                lhs[k * 128 : (k + 1) * 128, s * 128 : (s + 1) * 128] = (values * on).astype(BF)
        prod = jnp.dot(lhs[...], rhs[...], preferred_element_type=F32).astype(BF)
        for k in range(6):
            dst, r = divmod(k, 3)
            first = pl.multiple_of((group * 3 + r) * 256, 256)
            ab[dst * 128 : (dst + 1) * 128, pl.ds(first, 256)] = prod[k * 128 : (k + 1) * 128]
        return carry

    lax.fori_loop(0, 4, products, 0)

    for d in (1, 3, 2):
        weights_end(d)
    for d in range(4):
        for k, v in enumerate((y, ym, yp, y2)):
            got(WD + 4 * k + d, whole_block(d, v, 1 - c))

    own = None
    for dx in (2, 1, 3, 0):
        quarter = turn(x, dx, 4)
        cols = pl.ds(pl.multiple_of(quarter * 256, 256), 256)
        part = jnp.dot(
            ab[...], wb[:, :, :, :, cols].reshape(3072, 256), preferred_element_type=F32
        )
        pb[dx, 0] = part[:, 0:128].astype(BF)
        pb[dx, 1] = part[:, 128:256].astype(BF)
        for other in (1, 0):
            if dx == 0 and other == 0:
                continue
            zz = zh * 2 + (zl if other == 0 else 1 - zl)
            to = lax.rem(zz, 2)
            send(PT + dx * 2 + other, pb.at[dx, to], qb.at[dx, other], at(x_=quarter, z_=zz))
    got(GR, rb.at[x2, 0])
    got(GR + 1, rb.at[x2, 1])
    rb[x, 0] = sb[0, pl.ds(own_t, 2)]
    rb[x, 1] = sb[1, pl.ds(own_t, 2)]
    gate = jnp.zeros((256, 128), F32)
    for q in range(4):
        rows = jnp.concatenate([rb[q, 0].reshape(256, 128), rb[q, 1].reshape(256, 128)], axis=1)
        gate = gate + jnp.dot(rows, gw_ref[q * 256 : (q + 1) * 256, :], preferred_element_type=F32)
    gate_open = jax.nn.sigmoid(gate + gb_ref[...])
    hidden = sb[zl, pl.ds(own_t, 2)].reshape(256, 128).astype(F32)
    message = pb[0, zl].astype(F32)
    for dx in (0, 1, 3, 2):
        for other in (0, 1):
            if dx == 0 and other == 0:
                continue
            got(PT + dx * 2 + other, qb.at[dx, other])
            message = message + qb[dx, other].astype(F32)
    update = jnp.tanh(message + ub_ref[...])
    out_ref[...] = ((1.0 - gate_open) * hidden + gate_open * update).astype(BF)

    for d in pending:
        d.wait_send()
    for k in range(9):
        copy(WX + k, wz.at[0, 0], wb.at[0, 0, 0], dxp).wait_send()


def shards(state, rel_weight, gate_weight, gate_bias, update_bias, tile_values, tile_index, tile_count):
    src, dst, r = tile_index[0, 0], tile_index[0, 1], tile_index[0, 2]
    place = src // 16 * 16 + (src // 2) % 2 * 8 + (src // 4) % 4 * 2 + src % 2
    live = jnp.arange(16, dtype=jnp.int32) < tile_count[0, 0]
    target = jnp.where(live, dst * 3 + r, 6)
    meta = jnp.pad(jnp.stack([place, target]), ((0, 6), (0, 112)))
    vmem = pl.BlockSpec(memory_space=pltpu.VMEM)
    hbm = pl.BlockSpec(memory_space=pl.ANY)
    return pl.pallas_call(
        kernel,
        out_shape=jax.ShapeDtypeStruct((256, 128), BF),
        in_specs=[hbm] * 4 + [vmem] * 3,
        out_specs=vmem,
        scratch_shapes=[
            pltpu.VMEM((4, 16, 128, 128), BF),
            pltpu.VMEM((4, 8, 128), jnp.int32),
            pltpu.SMEM((4, 8, 128), jnp.int32),
            pltpu.VMEM((2, 64, 128, 128), BF),
            pltpu.VMEM((4, 2, 2, 128, 128), BF),
            pltpu.VMEM((4, 3, 32, 1024), BF),
            pltpu.VMEM((4, 3, 8, 32, 1024), BF),
            pltpu.VMEM((768, 2048), BF),
            pltpu.VMEM((2048, 256), BF),
            pltpu.VMEM((256, 3072), BF),
            pltpu.VMEM((4, 2, 256, 128), BF),
            pltpu.VMEM((4, 2, 256, 128), BF),
            pltpu.SemaphoreType.DMA((S.total,)),
            pltpu.SemaphoreType.DMA((S.total,)),
            pltpu.SemaphoreType.DMA((5,)),
        ],
        compiler_params=pltpu.CompilerParams(
            collective_id=0, has_side_effects=True, vmem_limit_bytes=48 * 1024 * 1024
        ),
    )(
        meta, state.reshape(2, 128, 128), rel_weight, tile_values[0], gate_weight,
        gate_bias.reshape(1, 128), update_bias.reshape(1, 128),
    )


def solution(mesh):
    from jax.sharding import PartitionSpec as P

    in_specs = (
        P("ent", "rel"),
        P("rel", "ent", None),
        P(None, "rel"),
        P("rel"),
        P("rel"),
        P("rel", "ent", None, None),
        P("rel", None, "ent"),
        P("rel", "ent"),
    )
    return jax.shard_map(
        shards, mesh=mesh, in_specs=in_specs, out_specs=P("ent", "rel"), check_vma=False
    )
```

```python
import jax
import jax.numpy as jnp
from jax import lax
from jax.experimental import pallas as pl
from jax.experimental.pallas import tpu as pltpu

MESH = pl.DeviceIdType.MESH
BF = jnp.bfloat16
F32 = jnp.float32


class Sems:
    def __init__(self):
        self.total = 0

    def take(self, count):
        first = self.total
        self.total += count
        return first


S = Sems()
TVP, TVM, TVR = S.take(2), S.take(2), S.take(2)
MET = S.take(3)
SY, SYR = S.take(2), S.take(2)
SZP, SZM = S.take(16), S.take(16)
SD = S.take(8)
GP, GM, GR = S.take(2), S.take(2), S.take(2)
WZP, WZM, WZR0, WZR1 = S.take(4), S.take(4), S.take(4), S.take(4)
WX = S.take(16)
DS = S.take(8)
WYP, WYM, WYR0, WYR1 = S.take(16), S.take(16), S.take(16), S.take(16)
WD = S.take(28)
PT = S.take(8)

QUARTERS = (2, 1, 3, 0)


def kernel(
    meta_in, state_in, relw_in, tv_in, gw_in, gb_in, ub_in, out_ref,
    gw_ref, gb_ref, ub_ref, gate_ref, tvb, metav, metas, sb, rb, wz, wb, cb, ab, pb, qb, ssem, rsem, lsem,
):
    rel = lax.axis_index("rel")
    ent = lax.axis_index("ent")
    x, zl = lax.div(rel, 2), lax.rem(rel, 2)
    zh, y, c = lax.div(ent, 8), lax.rem(lax.div(ent, 2), 4), lax.rem(ent, 2)
    z = zh * 2 + zl

    def turn(v, step, count):
        return lax.rem(v + (step + count) % count, count)

    def at(x_=None, y_=None, z_=None, c_=None):
        xx = x if x_ is None else x_
        yy = y if y_ is None else y_
        zz = z if z_ is None else z_
        cc = c if c_ is None else c_
        return (xx * 2 + lax.rem(zz, 2), lax.div(zz, 2) * 8 + yy * 2 + cc)

    xp, xm, x2 = turn(x, 1, 4), turn(x, -1, 4), turn(x, 2, 4)
    yp, ym, y2 = turn(y, 1, 4), turn(y, -1, 4), turn(y, 2, 4)
    hp, hm, h2 = turn(zh, 1, 4), turn(zh, -1, 4), turn(zh, 2, 4)
    zo = zh * 2 + (1 - zl)
    dxp, dxm, dx2 = at(x_=xp), at(x_=xm), at(x_=x2)
    dyp, dym = at(y_=yp), at(y_=ym)
    dzp, dzm = at(z_=turn(z, 1, 8)), at(z_=turn(z, -1, 8))
    dhp, dhm = at(z_=hp * 2 + zl), at(z_=hm * 2 + zl)
    dco = at(c_=1 - c)
    peers = [dxp, dxm, dx2, dyp, dym, dzp, dzm, dhp, dhm, dco]
    peers += [at(x_=v, z_=zo) for v in (xp, xm, x2)]
    away = zh != x
    targets = [at(x_=zh, z_=v * 2 + zl) for v in (h2, hp, hm, zh)]
    sources = [at(x_=v, z_=x * 2 + zl) for v in (x2, xp, xm, x)]

    pending = []

    def copy(i, src, dst, dev, there=None):
        return pltpu.make_async_remote_copy(
            src_ref=src, dst_ref=dst, send_sem=ssem.at[i],
            recv_sem=rsem.at[i if there is None else there],
            device_id=dev, device_id_type=MESH,
        )

    def send(i, src, dst, dev):
        d = copy(i, src, dst, dev)
        d.start()
        pending.append(d)

    def got(i, ref):
        copy(i, ref, ref, dco).wait_recv()

    yc = y * 2 + c
    own_t = ((zh * 2 + c) * 4 + y) * 2

    local = [
        pltpu.make_async_copy(state_in, sb.at[zl, pl.ds(own_t, 2)], lsem.at[1]),
        pltpu.make_async_copy(meta_in, metav.at[x], lsem.at[2]),
        pltpu.make_async_copy(tv_in, tvb.at[x], lsem.at[3]),
    ]
    for k in range(4):
        for j in range(2):
            cols = (turn(zh, QUARTERS[k], 4) * 2 + j) * 128
            local.append(
                pltpu.make_async_copy(
                    relw_in.at[:, :, pl.ds(pl.multiple_of(cols, 128), 128)],
                    wz.at[zh, k, j], lsem.at[8 + k * 2 + j],
                )
            )
    late = [
        pltpu.make_async_copy(gw_in, gw_ref, lsem.at[5]),
        pltpu.make_async_copy(gb_in, gb_ref, lsem.at[6]),
        pltpu.make_async_copy(ub_in, ub_ref, lsem.at[7]),
    ]
    for d in local + late:
        d.start()
    barrier = pltpu.get_barrier_semaphore()
    for dev in peers:
        pl.semaphore_signal(barrier, inc=1, device_id=dev, device_id_type=MESH)
    for dev in targets[:3] + sources[:3]:
        pl.semaphore_signal(barrier, inc=1, device_id=dev, device_id_type=MESH)

    @pl.when(away)
    def _():
        for dev in (targets[3], sources[3]):
            pl.semaphore_signal(barrier, inc=1, device_id=dev, device_id_type=MESH)

    for d in local:
        d.wait()
    pl.semaphore_wait(barrier, len(peers) + 6 + 2 * jnp.where(away, 1, 0))

    def weights_first(k):
        send(WZP + k, wz.at[zh, k], wz.at[zh, k], dhp)
        send(WZM + k, wz.at[zh, k], wz.at[zh, k], dhm)

    def weight_row(slot, k):
        d = lax.rem(slot - x + 4, 4)

        @pl.when(d != 0)
        def _():
            copy(
                WX + d * 4 + k, wz.at[slot, k], wb.at[k, :, x, :, yc], at(x_=slot)
            ).start()

    def weights_direct(k):
        to = WX + lax.rem(zh - x + 4, 4) * 4 + k
        for i in range(3):
            d = copy(DS + k * 4 + i, wz.at[zh, k], wb.at[k, :, x, :, yc], targets[i], to)
            d.start()
            pending.append(d)

        @pl.when(away)
        def _():
            copy(DS + k * 4 + 3, wz.at[zh, k], wb.at[k, :, x, :, yc], targets[3], to).start()

    def tv_half(x_, h):
        return tvb.at[x_, pl.ds(h * 8, 8)]

    order_y = (y, ym, yp, y2)

    def piece(step, j, cc=None, first=0, count=2):
        zz = turn(z, step, 8)
        place = (lax.div(zz, 2) * 2 + (c if cc is None else cc)) * 4 + order_y[j]
        return sb.at[lax.rem(zz, 2), pl.ds(place * 2 + first, count)]

    def chunk(step, cc):
        zz = turn(z, step, 8)
        return sb.at[lax.rem(zz, 2), pl.ds((lax.div(zz, 2) * 2 + cc) * 8, 8)]

    def share(k, step):
        send(SD + k, chunk(step, c), chunk(step, c), dco)

    def state_first(j):
        send(SZP + j, piece(0, j), piece(0, j), dzp)
        send(SZM + j, piece(0, j), piece(0, j), dzm)

    def state_on(k, j):
        got(SZP + (k - 1) * 4 + j, piece(-k, j))
        got(SZM + (k - 1) * 4 + j, piece(k, j))
        first, count = (0, 2) if k < 3 else (0, 1)
        ref = piece(-k, j, None, first, count)
        send(SZP + k * 4 + j, ref, ref, dzp)
        ref = piece(k, j, None, first if k < 3 else 1, count)
        send(SZM + k * 4 + j, ref, ref, dzm)

    def weights_far(k):
        got(WZP + k, wz.at[hm, k])
        send(WZR0 + k, wz.at[hm, k, 0], wz.at[hm, k, 0], dhp)
        got(WZM + k, wz.at[hp, k])
        send(WZR1 + k, wz.at[hp, k, 1], wz.at[hp, k, 1], dhm)
        weight_row(hm, k)
        weight_row(hp, k)

    def weights_last(k):
        got(WZR0 + k, wz.at[h2, k, 0])
        got(WZR1 + k, wz.at[h2, k, 1])
        weight_row(h2, k)

    def block(d, k, y_, cc=None):
        return wb.at[k, :, turn(x, -d, 4), :, y_ * 2 + (c if cc is None else cc)]

    def half_block(d, k, y_, h):
        return wb.at[k, h, turn(x, -d, 4), :, y_ * 2 + c]

    def all_blocks(k, y_, cc=None):
        return wb.at[k, :, :, :, y_ * 2 + (c if cc is None else cc)]

    def weights_out(d, k):
        dst = block(d, k, y)

        def spread(src):
            send(WYP + d * 4 + k, src, dst, dyp)
            send(WYM + d * 4 + k, src, dst, dym)
            send(WD + d * 4 + k, src, dst, dco)

        if d == 0 and k < 2:

            @pl.when(away)
            def _():
                got(WX + k, dst)
                spread(dst)
                del pending[-3:]

            @pl.when(jnp.logical_not(away))
            def _():
                spread(wz.at[x, k])
                del pending[-3:]

            for i in (WYP, WYM, WD):
                pending.append(copy(i + k, wz.at[x, k], dst, dco))
        elif d == 0:
            spread(wz.at[x, k])
        else:
            got(WX + d * 4 + k, dst)
            spread(dst)

    def weights_on(d, k):
        got(WYP + d * 4 + k, block(d, k, ym))
        send(WYR0 + d * 4 + k, half_block(d, k, ym, 0), half_block(d, k, ym, 0), dyp)
        got(WYM + d * 4 + k, block(d, k, yp))
        send(WYR1 + d * 4 + k, half_block(d, k, yp, 1), half_block(d, k, yp, 1), dym)

    def weights_end(d, k):
        got(WYR0 + d * 4 + k, half_block(d, k, y2, 0))
        got(WYR1 + d * 4 + k, half_block(d, k, y2, 1))

    groups = (0, 1, 3, 2)

    def outs(k):
        for d in groups:
            weights_out(d, k)

    def ons(k):
        for d in groups:
            weights_on(d, k)
        send(WD + 16 + k, all_blocks(k, ym), all_blocks(k, ym), dco)
        send(WD + 20 + k, all_blocks(k, yp), all_blocks(k, yp), dco)

    def ends(k):
        for d in groups:
            weights_end(d, k)
        send(WD + 24 + k, all_blocks(k, y2), all_blocks(k, y2), dco)

    def partner(k):
        for d in groups:
            got(WD + d * 4 + k, block(d, k, y, 1 - c))
        for i, v in enumerate((ym, yp, y2)):
            got(WD + 16 + 4 * i + k, all_blocks(k, v, 1 - c))

    weights_direct(0)
    mine = piece(0, 0)
    send(SY, mine, mine, dyp)
    send(SY + 1, mine, mine, dym)
    weights_direct(1)
    for k in (2, 3):
        weight_row(zh, k)
    weights_first(2)
    weights_first(3)
    state_first(0)
    for k, dev in enumerate((dxp, dxm, dx2)):
        send(MET + k, metav.at[x], metav.at[x], dev)
    send(TVP, tv_half(x, 0), tv_half(x, 0), dxp)
    send(TVM + 1, tv_half(x, 1), tv_half(x, 1), dxm)

    got(SY, piece(0, 1))
    send(SYR, piece(0, 1, None, 0, 1), piece(0, 1, None, 0, 1), dyp)
    got(SY + 1, piece(0, 2))
    send(SYR + 1, piece(0, 2, None, 1, 1), piece(0, 2, None, 1, 1), dym)

    outs(0)
    weights_far(2)
    state_first(1)
    state_first(2)
    weights_far(3)
    got(SYR, piece(0, 3, None, 0, 1))
    got(SYR + 1, piece(0, 3, None, 1, 1))
    state_first(3)
    share(0, 0)
    outs(1)
    weights_last(2)
    state_on(1, 0)
    weights_last(3)
    state_on(1, 1)
    state_on(1, 2)
    ons(0)
    state_on(1, 3)
    share(1, -1)
    share(2, 1)
    send(TVP + 1, tv_half(x, 1), tv_half(x, 1), dxp)
    send(TVM, tv_half(x, 0), tv_half(x, 0), dxm)
    for q in range(2):
        pair = sb.at[q, pl.ds(own_t, 2)]
        send(GP + q, pair, rb.at[x, q], dxp)
        send(GM + q, pair, rb.at[x, q], dxm)
    state_on(2, 0)
    outs(2)
    state_on(2, 1)
    state_on(2, 2)
    ons(1)
    state_on(2, 3)
    share(3, -2)
    share(4, 2)
    got(TVP, tv_half(xm, 0))
    send(TVR, tv_half(xm, 0), tv_half(xm, 0), dxp)
    got(TVM + 1, tv_half(xp, 1))
    send(TVR + 1, tv_half(xp, 1), tv_half(xp, 1), dxm)
    outs(3)
    state_on(3, 0)
    state_on(3, 1)
    for k in (2, 3):
        wb[k, :, x, :, yc] = wz[x, k]

    @pl.when(jnp.logical_not(away))
    def _():
        for k in (0, 1):
            wb[k, :, x, :, yc] = wz[x, k]

    cb[16] = jnp.zeros((128, 256), F32)
    for q in range(2):
        got(GP + q, rb.at[xm, q])
        got(GM + q, rb.at[xp, q])
    send(GR, rb.at[xm, 0], rb.at[xm, 0], dxp)
    send(GR + 1, rb.at[xp, 1], rb.at[xp, 1], dxm)
    ons(2)
    state_on(3, 2)
    state_on(3, 3)
    share(5, -3)
    share(6, 3)
    ends(0)
    for k, v in enumerate((xm, xp, x2)):
        got(MET + k, metav.at[v])
    listing = pltpu.make_async_copy(metav, metas, lsem.at[4])
    listing.start()
    ons(3)
    ends(1)
    got(GR, rb.at[x2, 0])
    got(GR + 1, rb.at[x2, 1])
    rb[x, 0] = sb[0, pl.ds(own_t, 2)]
    rb[x, 1] = sb[1, pl.ds(own_t, 2)]
    for d in late:
        d.wait()
    gate = jnp.zeros((256, 128), F32)
    for q in range(4):
        rows = jnp.concatenate([rb[q, 0].reshape(256, 128), rb[q, 1].reshape(256, 128)], axis=1)
        gate = gate + jnp.dot(rows, gw_ref[q * 256 : (q + 1) * 256, :], preferred_element_type=F32)
    gate_ref[...] = jax.nn.sigmoid(gate + gb_ref[...])
    for j in range(4):
        got(SZP + 12 + j, piece(4, j, None, 0, 1))
        got(SZM + 12 + j, piece(4, j, None, 1, 1))
    share(7, 4)
    got(TVP + 1, tv_half(xm, 1))
    got(TVM, tv_half(xp, 0))
    got(TVR, tv_half(x2, 0))
    got(TVR + 1, tv_half(x2, 1))
    for k, step in enumerate((0, -1, 1, -2, 2, -3, 3, 4)):
        got(SD + k, chunk(step, 1 - c))
    listing.wait()

    def products(group, carry):
        last = [jnp.int32(16)] * 6
        for t in range(16):
            src = metas[group, 0, t]
            cls = metas[group, 1, t]
            prev = jnp.int32(16)
            for k in range(6):
                prev = jnp.where(cls == k, last[k], prev)
                last[k] = jnp.where(cls == k, t, last[k])
            rows = jnp.concatenate([sb[0, src], sb[1, src]], axis=1)
            cb[t] = jnp.dot(tvb[group, t], rows, preferred_element_type=F32) + cb[prev]
        for k in range(6):
            dst, r = divmod(k, 3)
            first = pl.multiple_of((group * 3 + r) * 256, 256)
            ab[dst * 128 : (dst + 1) * 128, pl.ds(first, 256)] = cb[last[k]].astype(BF)
        return carry

    lax.fori_loop(0, 4, products, 0)

    for k, dx in enumerate(QUARTERS):
        if k >= 2:
            ends(k)
        partner(k)
        quarter = turn(x, dx, 4)
        cols = jnp.concatenate([wb[k, 0].reshape(3072, 128), wb[k, 1].reshape(3072, 128)], axis=1)
        part = jnp.dot(ab[...], cols, preferred_element_type=F32)
        pb[dx, 0] = part[:, 0:128].astype(BF)
        pb[dx, 1] = part[:, 128:256].astype(BF)
        for other in (1, 0):
            if dx == 0 and other == 0:
                continue
            zz = zh * 2 + (zl if other == 0 else 1 - zl)
            to = lax.rem(zz, 2)
            send(PT + dx * 2 + other, pb.at[dx, to], qb.at[dx, other], at(x_=quarter, z_=zz))
    hidden = sb[zl, pl.ds(own_t, 2)].reshape(256, 128).astype(F32)
    message = pb[0, zl].astype(F32)
    for dx in QUARTERS:
        for other in (0, 1):
            if dx == 0 and other == 0:
                continue
            got(PT + dx * 2 + other, qb.at[dx, other])
            message = message + qb[dx, other].astype(F32)
    update = jnp.tanh(message + ub_ref[...])
    gate_open = gate_ref[...]
    out_ref[...] = ((1.0 - gate_open) * hidden + gate_open * update).astype(BF)

    for d in pending:
        d.wait_send()
    for d in range(1, 4):
        for k in (2, 3):
            copy(WX + d * 4 + k, wz.at[0, 0], wb.at[0, :, 0, :, 0], dxp).wait_send()

    @pl.when(away)
    def _():
        for k in (0, 1):
            copy(DS + k * 4 + 3, wz.at[0, 0], wb.at[0, :, 0, :, 0], dxp).wait_send()


def shards(state, rel_weight, gate_weight, gate_bias, update_bias, tile_values, tile_index, tile_count):
    src, dst, r = tile_index[0, 0], tile_index[0, 1], tile_index[0, 2]
    place = src // 16 * 16 + (src // 2) % 2 * 8 + (src // 4) % 4 * 2 + src % 2
    live = jnp.arange(16, dtype=jnp.int32) < tile_count[0, 0]
    target = jnp.where(live, dst * 3 + r, 6)
    meta = jnp.pad(jnp.stack([place, target]), ((0, 6), (0, 112)))
    vmem = pl.BlockSpec(memory_space=pltpu.VMEM)
    hbm = pl.BlockSpec(memory_space=pl.ANY)
    return pl.pallas_call(
        kernel,
        out_shape=jax.ShapeDtypeStruct((256, 128), BF),
        in_specs=[hbm] * 7,
        out_specs=vmem,
        scratch_shapes=[
            pltpu.VMEM((1024, 128), BF),
            pltpu.VMEM((1, 128), F32),
            pltpu.VMEM((1, 128), F32),
            pltpu.VMEM((256, 128), F32),
            pltpu.VMEM((4, 16, 128, 128), BF),
            pltpu.VMEM((4, 8, 128), jnp.int32),
            pltpu.SMEM((4, 8, 128), jnp.int32),
            pltpu.VMEM((2, 64, 128, 128), BF),
            pltpu.VMEM((4, 2, 2, 128, 128), BF),
            pltpu.VMEM((4, 4, 2, 3, 32, 128), BF),
            pltpu.VMEM((4, 2, 4, 3, 8, 32, 128), BF),
            pltpu.VMEM((17, 128, 256), F32),
            pltpu.VMEM((256, 3072), BF),
            pltpu.VMEM((4, 2, 256, 128), BF),
            pltpu.VMEM((4, 2, 256, 128), BF),
            pltpu.SemaphoreType.DMA((S.total,)),
            pltpu.SemaphoreType.DMA((S.total,)),
            pltpu.SemaphoreType.DMA((16,)),
        ],
        compiler_params=pltpu.CompilerParams(
            collective_id=0, has_side_effects=True, vmem_limit_bytes=62 * 1024 * 1024
        ),
    )(
        meta, state.reshape(2, 128, 128), rel_weight, tile_values[0], gate_weight,
        gate_bias.reshape(1, 128), update_bias.reshape(1, 128),
    )


def solution(mesh):
    from jax.sharding import PartitionSpec as P

    in_specs = (
        P("ent", "rel"),
        P("rel", "ent", None),
        P(None, "rel"),
        P("rel"),
        P("rel"),
        P("rel", "ent", None, None),
        P("rel", None, "ent"),
        P("rel", "ent"),
    )
    return jax.shard_map(
        shards, mesh=mesh, in_specs=in_specs, out_specs=P("ent", "rel"), check_vma=False
    )
```

```python
import jax
import jax.numpy as jnp
from jax import lax
from jax.experimental import pallas as pl
from jax.experimental.pallas import tpu as pltpu

MESH = pl.DeviceIdType.MESH
BF = jnp.bfloat16
F32 = jnp.float32


class Sems:
    def __init__(self):
        self.total = 0

    def take(self, count):
        first = self.total
        self.total += count
        return first


S = Sems()
TVP, TVM, TVR = S.take(4), S.take(4), S.take(4)
MET = S.take(3)
SY, SYR = S.take(2), S.take(2)
SZP, SZM = S.take(16), S.take(16)
SD, SE = S.take(8), S.take(8)
VZP, VZM = S.take(4), S.take(4)
VYP, VYM, VYR0, VYR1 = S.take(8), S.take(8), S.take(8), S.take(8)
GP, GM, GR = S.take(2), S.take(2), S.take(2)
WZP, WZM, WZR0, WZR1 = S.take(4), S.take(4), S.take(4), S.take(4)
WX = S.take(12)
WYP, WYM, WYR0, WYR1 = S.take(16), S.take(16), S.take(16), S.take(16)
WD = S.take(28)
PT = S.take(8)

QUARTERS = (2, 1, 3, 0)


def kernel(
    meta_in, state_in, relw_in, tv_in, gw_in, gb_in, ub_in, out_ref,
    gw_ref, gb_ref, ub_ref, gate_ref, tvb, metav, metas, sb, rb, wz, wb, cb, ab, pb, qb, ssem, rsem, lsem,
):
    rel = lax.axis_index("rel")
    ent = lax.axis_index("ent")
    x, zl = lax.div(rel, 2), lax.rem(rel, 2)
    zh, y, c = lax.div(ent, 8), lax.rem(lax.div(ent, 2), 4), lax.rem(ent, 2)
    z = zh * 2 + zl

    def turn(v, step, count):
        return lax.rem(v + (step + count) % count, count)

    def at(x_=None, y_=None, z_=None, c_=None):
        xx = x if x_ is None else x_
        yy = y if y_ is None else y_
        zz = z if z_ is None else z_
        cc = c if c_ is None else c_
        return (xx * 2 + lax.rem(zz, 2), lax.div(zz, 2) * 8 + yy * 2 + cc)

    xp, xm, x2 = turn(x, 1, 4), turn(x, -1, 4), turn(x, 2, 4)
    yp, ym, y2 = turn(y, 1, 4), turn(y, -1, 4), turn(y, 2, 4)
    hp, hm, h2 = turn(zh, 1, 4), turn(zh, -1, 4), turn(zh, 2, 4)
    zo = zh * 2 + (1 - zl)
    dxp, dxm, dx2 = at(x_=xp), at(x_=xm), at(x_=x2)
    dyp, dym = at(y_=yp), at(y_=ym)
    dzp, dzm = at(z_=turn(z, 1, 8)), at(z_=turn(z, -1, 8))
    dhp, dhm = at(z_=hp * 2 + zl), at(z_=hm * 2 + zl)
    dco = at(c_=1 - c)
    peers = [dxp, dxm, dx2, dyp, dym, dzp, dzm, dhp, dhm, dco]
    peers += [at(x_=v, z_=zo) for v in (xp, xm, x2)]

    pending = []

    def copy(i, src, dst, dev):
        return pltpu.make_async_remote_copy(
            src_ref=src, dst_ref=dst, send_sem=ssem.at[i], recv_sem=rsem.at[i],
            device_id=dev, device_id_type=MESH,
        )

    def send(i, src, dst, dev):
        d = copy(i, src, dst, dev)
        d.start()
        pending.append(d)

    def got(i, ref):
        copy(i, ref, ref, dco).wait_recv()

    yc = y * 2 + c
    own = zh * 2 + c

    local = [
        pltpu.make_async_copy(state_in, sb.at[zl, own, y], lsem.at[1]),
        pltpu.make_async_copy(meta_in, metav.at[x], lsem.at[2]),
        pltpu.make_async_copy(tv_in, tvb.at[x], lsem.at[3]),
    ]
    for k in range(4):
        for j in range(2):
            cols = (turn(zh, QUARTERS[k], 4) * 2 + j) * 128
            local.append(
                pltpu.make_async_copy(
                    relw_in.at[:, :, pl.ds(pl.multiple_of(cols, 128), 128)],
                    wz.at[zh, k, j], lsem.at[8 + k * 2 + j],
                )
            )
    late = [
        pltpu.make_async_copy(gw_in, gw_ref, lsem.at[5]),
        pltpu.make_async_copy(gb_in, gb_ref, lsem.at[6]),
        pltpu.make_async_copy(ub_in, ub_ref, lsem.at[7]),
    ]
    for d in local + late:
        d.start()
    barrier = pltpu.get_barrier_semaphore()
    for dev in peers:
        pl.semaphore_signal(barrier, inc=1, device_id=dev, device_id_type=MESH)
    for d in local:
        d.wait()
    pl.semaphore_wait(barrier, len(peers))

    def weights_first(k):
        send(WZP + k, wz.at[zh, k], wz.at[zh, k], dhp)
        send(WZM + k, wz.at[zh, k], wz.at[zh, k], dhm)

    def weight_row(slot, k):
        d = lax.rem(slot - x + 4, 4)

        @pl.when(d != 0)
        def _():
            copy(
                WX + (d - 1) * 4 + k, wz.at[slot, k], wb.at[k, :, x, :, yc], at(x_=slot)
            ).start()

    def tv_part(x_, h):
        return tvb.at[x_, pl.ds(h * 4, 4)]

    order_y = (y, ym, yp, y2)

    def tile(step, j, i):
        zz = turn(z, step, 8)
        rows = 3 if i == 1 else pl.ds(0, 3)
        return sb.at[lax.rem(zz, 2), lax.div(zz, 2) * 2 + c, order_y[j], rows]

    def half_tile(step, j, i, h):
        zz = turn(z, step, 8)
        place = (lax.rem(zz, 2), lax.div(zz, 2) * 2 + c, order_y[j])
        if i == 1:
            return sb.at[*place, 3, pl.ds(h * 32, 32)]
        long_first = j in (0, 3)
        cut = 2 if long_first else 1
        return sb.at[*place, pl.ds(0, cut) if h == 0 else pl.ds(cut, 3 - cut)]

    def tiles(step, i, cc):
        zz = turn(z, step, 8)
        rows = 3 if i == 1 else pl.ds(0, 3)
        return sb.at[lax.rem(zz, 2), lax.div(zz, 2) * 2 + cc, :, rows]

    def share(k, step):
        send(SD + k, tiles(step, 0, c), tiles(step, 0, c), dco)

    def y_part(y_, h):
        return sb.at[zl, own, y_, pl.ds(0, 2) if h == 0 else 2]

    def state_first(j):
        send(SZP + j, tile(0, j, 0), tile(0, j, 0), dzp)
        send(SZM + j, tile(0, j, 0), tile(0, j, 0), dzm)

    def state_on(k, j):
        got(SZP + (k - 1) * 4 + j, tile(-k, j, 0))
        got(SZM + (k - 1) * 4 + j, tile(k, j, 0))
        left = tile(-k, j, 0) if k < 3 else half_tile(-k, j, 0, 0)
        right = tile(k, j, 0) if k < 3 else half_tile(k, j, 0, 1)
        send(SZP + k * 4 + j, left, left, dzp)
        send(SZM + k * 4 + j, right, right, dzm)

    steps = (0, -1, 1, -2, 2, -3, 3, 4)

    def second_y(n):
        ref = tile(steps[n], 0, 1)
        send(VYP + n, ref, ref, dyp)
        send(VYM + n, ref, ref, dym)

    def second_z(k):
        got(VZP + k - 1, tile(-k, 0, 1))
        got(VZM + k - 1, tile(k, 0, 1))
        left = tile(-k, 0, 1) if k < 3 else half_tile(-k, 0, 1, 0)
        right = tile(k, 0, 1) if k < 3 else half_tile(k, 0, 1, 1)
        send(VZP + k, left, left, dzp)
        send(VZM + k, right, right, dzm)
        second_y(2 * k - 1)
        second_y(2 * k)

    def second_on(n):
        got(VYP + n, tile(steps[n], 1, 1))
        ref = half_tile(steps[n], 1, 1, 0)
        send(VYR0 + n, ref, ref, dyp)
        got(VYM + n, tile(steps[n], 2, 1))
        ref = half_tile(steps[n], 2, 1, 1)
        send(VYR1 + n, ref, ref, dym)

    def second_end(n):
        got(VYR0 + n, half_tile(steps[n], 3, 1, 0))
        got(VYR1 + n, half_tile(steps[n], 3, 1, 1))
        send(SE + n, tiles(steps[n], 1, c), tiles(steps[n], 1, c), dco)

    def weights_far(k):
        got(WZP + k, wz.at[hm, k])
        send(WZR0 + k, wz.at[hm, k, 0], wz.at[hm, k, 0], dhp)
        got(WZM + k, wz.at[hp, k])
        send(WZR1 + k, wz.at[hp, k, 1], wz.at[hp, k, 1], dhm)
        weight_row(hm, k)
        weight_row(hp, k)

    def weights_last(k):
        got(WZR0 + k, wz.at[h2, k, 0])
        got(WZR1 + k, wz.at[h2, k, 1])
        weight_row(h2, k)

    def block(d, k, y_, cc=None):
        return wb.at[k, :, turn(x, -d, 4), :, y_ * 2 + (c if cc is None else cc)]

    def half_block(d, k, y_, h):
        return wb.at[k, h, turn(x, -d, 4), :, y_ * 2 + c]

    def all_blocks(k, y_, cc=None):
        return wb.at[k, :, :, :, y_ * 2 + (c if cc is None else cc)]

    def weights_out(d, k):
        src = block(d, k, y)
        if d == 0:
            src = wz.at[x, k]
        else:
            got(WX + (d - 1) * 4 + k, src)
        send(WYP + d * 4 + k, src, block(d, k, y), dyp)
        send(WYM + d * 4 + k, src, block(d, k, y), dym)
        send(WD + d * 4 + k, src, block(d, k, y), dco)

    def weights_on(d, k):
        got(WYP + d * 4 + k, block(d, k, ym))
        send(WYR0 + d * 4 + k, half_block(d, k, ym, 0), half_block(d, k, ym, 0), dyp)
        got(WYM + d * 4 + k, block(d, k, yp))
        send(WYR1 + d * 4 + k, half_block(d, k, yp, 1), half_block(d, k, yp, 1), dym)

    def weights_end(d, k):
        got(WYR0 + d * 4 + k, half_block(d, k, y2, 0))
        got(WYR1 + d * 4 + k, half_block(d, k, y2, 1))

    groups = (0, 1, 3, 2)

    def outs(k):
        for d in groups:
            weights_out(d, k)

    def ons(k):
        for d in groups:
            weights_on(d, k)
        send(WD + 16 + k, all_blocks(k, ym), all_blocks(k, ym), dco)
        send(WD + 20 + k, all_blocks(k, yp), all_blocks(k, yp), dco)

    def ends(k):
        for d in groups:
            weights_end(d, k)
        send(WD + 24 + k, all_blocks(k, y2), all_blocks(k, y2), dco)

    def partner(k):
        for d in groups:
            got(WD + d * 4 + k, block(d, k, y, 1 - c))
        for i, v in enumerate((ym, yp, y2)):
            got(WD + 16 + 4 * i + k, all_blocks(k, v, 1 - c))

    def tv_send(n):
        right, left = n, (n + 2) % 4
        send(TVP + right, tv_part(x, right), tv_part(x, right), dxp)
        send(TVM + left, tv_part(x, left), tv_part(x, left), dxm)

    def tv_on(n):
        got(TVP + n, tv_part(xm, n))
        send(TVR + n, tv_part(xm, n), tv_part(xm, n), dxp)
        got(TVM + 2 + n, tv_part(xp, 2 + n))
        send(TVR + 2 + n, tv_part(xp, 2 + n), tv_part(xp, 2 + n), dxm)

    def tv_end():
        for n in range(2):
            got(TVP + 2 + n, tv_part(xm, 2 + n))
            got(TVM + n, tv_part(xp, n))
        for n in range(4):
            got(TVR + n, tv_part(x2, n))

    def gate_first():
        for q in range(2):
            pair = sb.at[q, own, y]
            send(GP + q, pair, rb.at[x, q], dxp)
            send(GM + q, pair, rb.at[x, q], dxm)

    def gate_on():
        for q in range(2):
            got(GP + q, rb.at[xm, q])
            got(GM + q, rb.at[xp, q])
        send(GR, rb.at[xm, 0], rb.at[xm, 0], dxp)
        send(GR + 1, rb.at[xp, 1], rb.at[xp, 1], dxm)

    def gate_end():
        got(GR, rb.at[x2, 0])
        got(GR + 1, rb.at[x2, 1])
        rb[x, 0] = sb[0, own, y]
        rb[x, 1] = sb[1, own, y]
        for d in late:
            d.wait()
        gate = jnp.zeros((256, 128), F32)
        for q in range(4):
            rows = jnp.concatenate(
                [rb[q, 0].reshape(256, 128), rb[q, 1].reshape(256, 128)], axis=1
            )
            gate = gate + jnp.dot(
                rows, gw_ref[q * 256 : (q + 1) * 256, :], preferred_element_type=F32
            )
        gate_ref[...] = jax.nn.sigmoid(gate + gb_ref[...])

    listing = pltpu.make_async_copy(metav, metas, lsem.at[4])

    def products(group, carry):
        last = [jnp.int32(16)] * 6
        for t in range(16):
            row, part, half = metas[group, 0, t], metas[group, 1, t], metas[group, 2, t]
            cls = metas[group, 3, t]
            prev = jnp.int32(16)
            for k in range(6):
                prev = jnp.where(cls == k, last[k], prev)
                last[k] = jnp.where(cls == k, t, last[k])
            pair = [sb[q, row, part, pl.ds(half * 2, 2)].reshape(128, 128) for q in range(2)]
            rows = jnp.concatenate(pair, axis=1)
            cb[t] = jnp.dot(tvb[group, t], rows, preferred_element_type=F32) + cb[prev]
        for k in range(6):
            dst, r = divmod(k, 3)
            first = pl.multiple_of((group * 3 + r) * 256, 256)
            ab[dst * 128 : (dst + 1) * 128, pl.ds(first, 256)] = cb[last[k]].astype(BF)
        return carry

    def message_out(k):
        partner(k)
        dx = QUARTERS[k]
        quarter = turn(x, dx, 4)
        cols = jnp.concatenate([wb[k, 0].reshape(3072, 128), wb[k, 1].reshape(3072, 128)], axis=1)
        part = jnp.dot(ab[...], cols, preferred_element_type=F32)
        pb[dx, 0] = part[:, 0:128].astype(BF)
        pb[dx, 1] = part[:, 128:256].astype(BF)
        for other in (1, 0):
            if dx == 0 and other == 0:
                continue
            zz = zh * 2 + (zl if other == 0 else 1 - zl)
            to = lax.rem(zz, 2)
            send(PT + dx * 2 + other, pb.at[dx, to], qb.at[dx, other], at(x_=quarter, z_=zz))

    def state_end():
        for k, step in enumerate(steps):
            got(SD + k, tiles(step, 0, 1 - c))
            got(SE + k, tiles(step, 1, 1 - c))

    send(VZP, tile(0, 0, 1), tile(0, 0, 1), dzp)
    send(VZM, tile(0, 0, 1), tile(0, 0, 1), dzm)
    weights_first(0)
    weights_first(1)
    send(SY, tile(0, 0, 0), tile(0, 0, 0), dyp)
    send(SY + 1, tile(0, 0, 0), tile(0, 0, 0), dym)
    second_y(0)
    for k in range(4):
        weight_row(zh, k)
    for k, dev in enumerate((dxp, dxm, dx2)):
        send(MET + k, metav.at[x], metav.at[x], dev)
    tv_send(0)
    got(SY, tile(0, 1, 0))
    send(SYR, y_part(ym, 0), y_part(ym, 0), dyp)
    got(SY + 1, tile(0, 2, 0))
    send(SYR + 1, y_part(yp, 1), y_part(yp, 1), dym)
    second_z(1)
    weights_far(0)
    tv_send(1)
    weights_first(2)
    second_on(0)
    state_first(0)
    second_z(2)
    weights_far(1)
    tv_send(2)
    weights_first(3)
    state_first(1)
    state_first(2)
    got(SYR, y_part(y2, 0))
    got(SYR + 1, y_part(y2, 1))
    second_z(3)
    second_on(1)
    second_on(2)
    weights_last(0)
    weights_out(0, 0)
    weights_far(2)
    state_first(3)
    state_on(1, 0)
    for d in (1, 3, 2):
        weights_out(d, 0)
    weights_last(1)
    weights_far(3)
    got(VZP + 3, half_tile(4, 0, 1, 0))
    got(VZM + 3, half_tile(4, 0, 1, 1))
    second_y(7)
    second_on(3)
    second_on(4)
    state_on(1, 1)
    state_on(1, 2)
    outs(1)
    weights_last(2)
    state_on(1, 3)
    gate_first()
    tv_send(3)
    weights_last(3)
    ons(0)
    state_on(2, 0)
    state_on(2, 1)
    second_on(5)
    second_on(6)
    outs(2)
    state_on(2, 2)
    state_on(2, 3)
    tv_on(0)
    second_on(7)
    for k in range(5):
        share(k, steps[k])
    ons(1)
    tv_on(1)
    state_on(3, 0)
    state_on(3, 1)
    outs(3)
    state_on(3, 2)
    state_on(3, 3)
    share(5, -3)
    share(6, 3)
    for n in range(8):
        second_end(n)
    ends(0)
    gate_on()
    for k in range(4):
        wb[k, :, x, :, yc] = wz[x, k]
    cb[16] = jnp.zeros((128, 256), F32)
    for k, v in enumerate((xm, xp, x2)):
        got(MET + k, metav.at[v])
    listing.start()
    ons(2)
    for j in range(4):
        got(SZP + 12 + j, half_tile(4, j, 0, 0))
        got(SZM + 12 + j, half_tile(4, j, 0, 1))
    share(7, 4)
    ends(1)
    tv_end()
    state_end()
    listing.wait()
    lax.fori_loop(0, 4, products, 0)
    ons(3)
    message_out(0)
    gate_end()
    message_out(1)
    ends(2)
    message_out(2)
    ends(3)
    message_out(3)

    hidden = sb[zl, own, y].reshape(256, 128).astype(F32)
    message = pb[0, zl].astype(F32)
    for dx in QUARTERS:
        for other in (0, 1):
            if dx == 0 and other == 0:
                continue
            got(PT + dx * 2 + other, qb.at[dx, other])
            message = message + qb[dx, other].astype(F32)
    update = jnp.tanh(message + ub_ref[...])
    gate_open = gate_ref[...]
    out_ref[...] = ((1.0 - gate_open) * hidden + gate_open * update).astype(BF)

    for d in pending:
        d.wait_send()
    for k in range(12):
        copy(WX + k, wz.at[0, 0], wb.at[0, :, 0, :, 0], dxp).wait_send()


def shards(state, rel_weight, gate_weight, gate_bias, update_bias, tile_values, tile_index, tile_count):
    src, dst, r = tile_index[0, 0], tile_index[0, 1], tile_index[0, 2]
    place = [src // 16 * 2 + (src // 2) % 2, (src // 4) % 4, src % 2]
    live = jnp.arange(16, dtype=jnp.int32) < tile_count[0, 0]
    target = jnp.where(live, dst * 3 + r, 6)
    meta = jnp.pad(jnp.stack(place + [target]), ((0, 4), (0, 112)))
    vmem = pl.BlockSpec(memory_space=pltpu.VMEM)
    hbm = pl.BlockSpec(memory_space=pl.ANY)
    return pl.pallas_call(
        kernel,
        out_shape=jax.ShapeDtypeStruct((256, 128), BF),
        in_specs=[hbm] * 7,
        out_specs=vmem,
        scratch_shapes=[
            pltpu.VMEM((1024, 128), BF),
            pltpu.VMEM((1, 128), F32),
            pltpu.VMEM((1, 128), F32),
            pltpu.VMEM((256, 128), F32),
            pltpu.VMEM((4, 16, 128, 128), BF),
            pltpu.VMEM((4, 8, 128), jnp.int32),
            pltpu.SMEM((4, 8, 128), jnp.int32),
            pltpu.VMEM((2, 8, 4, 4, 64, 128), BF),
            pltpu.VMEM((4, 2, 4, 64, 128), BF),
            pltpu.VMEM((4, 4, 2, 3, 32, 128), BF),
            pltpu.VMEM((4, 2, 4, 3, 8, 32, 128), BF),
            pltpu.VMEM((17, 128, 256), F32),
            pltpu.VMEM((256, 3072), BF),
            pltpu.VMEM((4, 2, 256, 128), BF),
            pltpu.VMEM((4, 2, 256, 128), BF),
            pltpu.SemaphoreType.DMA((S.total,)),
            pltpu.SemaphoreType.DMA((S.total,)),
            pltpu.SemaphoreType.DMA((16,)),
        ],
        compiler_params=pltpu.CompilerParams(
            collective_id=0, has_side_effects=True, vmem_limit_bytes=62 * 1024 * 1024
        ),
    )(
        meta, state.reshape(4, 64, 128), rel_weight, tile_values[0], gate_weight,
        gate_bias.reshape(1, 128), update_bias.reshape(1, 128),
    )


def solution(mesh):
    from jax.sharding import PartitionSpec as P

    in_specs = (
        P("ent", "rel"),
        P("rel", "ent", None),
        P(None, "rel"),
        P("rel"),
        P("rel"),
        P("rel", "ent", None, None),
        P("rel", None, "ent"),
        P("rel", "ent"),
    )
    return jax.shard_map(
        shards, mesh=mesh, in_specs=in_specs, out_specs=P("ent", "rel"), check_vma=False
    )
```
